128 devices in a mesh: expert: 8 (over z_lo, x), shard: 16 (over z_hi, y, core).
Axes of the slice: x: 4, y: 4, z: 4 (z_hi: 2, z_lo: 2; z = z_hi * 2 + z_lo), core: 2. Of those that a mesh axis runs over, the one named last changes fastest.
Arguments:
- master_gate: float32 [128, 2048, 768], P('expert', 'shard'), may hold values from -0.1875 to 0.1875
- second_gate: bfloat16 [128, 2048, 768], P('expert', 'shard'), may hold values from -0.0625 to 0.0625
- master_up: float32 [128, 2048, 768], P('expert', 'shard'), may hold values from -0.1875 to 0.1875
- second_up: bfloat16 [128, 2048, 768], P('expert', 'shard'), may hold values from -0.0625 to 0.0625
- router_weight: float32 [2048, 128], P('shard', 'expert'), may hold values from -0.125 to 0.125
- router_gain: float32 [2048], P('shard'), may hold values from 0.25 to 1.75
Outputs:
- final_gate: bfloat16 [128, 2048, 768], P(('expert', 'shard'))
- final_up: bfloat16 [128, 2048, 768], P(('expert', 'shard'))
- scale_gate: float32 [128, 768], P(('expert', 'shard'))
- scale_up: float32 [128, 768], P(('expert', 'shard'))
- serve_router: bfloat16 [2048, 128], replicated
The draws below stay inside these ranges and needn't reach their ends.
All inputs are finite; a program needn't handle non-finite values. Where the reference program divides by a largest or mean magnitude, that divisor is 1e-20 or more.
Results may differ from the reference program's by a relative error of at most 0.0085.
Values may be sent and summed in bfloat16 or wider, within the bound.
No kernel may reach another device: no remote copies, remote signals or barrier semaphores. Data moves between devices by JAX's collectives and lax.ppermute only.
A program may use at most 128 MiB of HBM per device.

```python
import jax
import jax.numpy as jnp

EXPERTS = 128
D_MODEL = 2048
D_EXPERT = 768


def raised(entries, rng, source, target, shards_of, factor):
    def block_of(position):
        return (jnp.arange(entries.shape[position]) // (entries.shape[position] // shards_of)).reshape((-1,) + (1,) * (entries.ndim - 1 - position))

    first = jax.random.permutation(rng, shards_of)[block_of(target)]
    other_side = (block_of(target) + shards_of // 2) % shards_of
    return jnp.where((block_of(source) == first) | (block_of(source) == other_side), factor * entries, entries)


def block_levels(stream_key, extent, split, low, top_value):
    factor_of, own = 1.0, jax.random.fold_in(stream_key, 6)
    for dim, blocks in split:
        steps = jnp.exp(jax.random.uniform(jax.random.fold_in(own, dim), (blocks,), jnp.float32, low / len(split), top_value / len(split)))
        factor_of = factor_of * jnp.repeat(steps, extent[dim] // blocks).reshape([-1 if axis == dim else 1 for axis in range(len(extent))])
    return factor_of


def normal_values(own_key, dims, scale, bound, cuts=(), held_as=jnp.bfloat16):
    loudness = block_levels(own_key, dims, cuts, -0.22, 0.18) if cuts else 1.0
    result = jax.random.normal(own_key, dims, jnp.float32) * scale * loudness
    return jnp.minimum(jnp.maximum(result, -bound), bound).astype(held_as)


def noise_with(key, shape, width, most, split, heavy, dtype=jnp.bfloat16):
    entries = width * jax.random.normal(key, shape, jnp.float32)
    if split:
        entries = entries * block_levels(key, shape, split, -0.22, 0.18)
    return jnp.clip(raised(entries, jax.random.fold_in(key, 3), *heavy), -most, most).astype(dtype)


def setup_inputs(seed: int = 0) -> dict:
    key_of = jax.random.split(jax.random.key(seed), 7)
    master_gate = noise_with(key_of[0], (EXPERTS, D_MODEL, D_EXPERT), D_MODEL ** -0.5, 0.1875, ((0, 8), (1, 16)), (1, 2, 16, 2.0), jnp.float32)
    second_gate = normal_values(key_of[1], (EXPERTS, D_MODEL, D_EXPERT), (D_MODEL * 4) ** -0.5, 0.0625, ((0, 8), (1, 16)))
    master_up = noise_with(key_of[2], (EXPERTS, D_MODEL, D_EXPERT), D_MODEL ** -0.5, 0.1875, ((0, 8), (1, 16)), (1, 2, 16, 2.0), jnp.float32)
    second_up = normal_values(key_of[3], (EXPERTS, D_MODEL, D_EXPERT), (D_MODEL * 4) ** -0.5, 0.0625, ((0, 8), (1, 16)))
    router_weight = normal_values(key_of[4], (D_MODEL, EXPERTS), D_MODEL ** -0.5, 0.125, ((0, 16), (1, 8)), jnp.float32)
    router_gain = jnp.clip(1.0 + 0.15 * jax.random.normal(key_of[5], (D_MODEL,), jnp.float32), 0.25, 1.75)
    return {"master_gate": master_gate, "second_gate": second_gate, "master_up": master_up, "second_up": second_up, "router_weight": router_weight, "router_gain": router_gain}


def reference(master_gate, second_gate, master_up, second_up, router_weight, router_gain):
    merged_gate = master_gate + second_gate.astype(jnp.float32)
    merged_up = master_up + second_up.astype(jnp.float32)
    scale_gate = jnp.sum(jnp.abs(merged_gate), axis=1) / D_MODEL
    final_gate = (merged_gate / jnp.expand_dims(scale_gate, 1)).astype(jnp.bfloat16)
    scale_up = jnp.sum(jnp.abs(merged_up), axis=1) / D_MODEL
    final_up = (merged_up / jnp.expand_dims(scale_up, 1)).astype(jnp.bfloat16)
    serve_router = (router_weight * router_gain[:, None]).astype(jnp.bfloat16)
    return final_gate, final_up, scale_gate, scale_up, serve_router
```

```python
from itertools import product

import jax
import jax.numpy as jnp
from jax import lax
from jax.experimental import pallas as pl
from jax.experimental.pallas import tpu as pltpu
from jax.sharding import Mesh
from jax.sharding import PartitionSpec as P


D_MODEL = 2048
LANES = 128
EXPERT = ("zl", "x")
SHARD = ("zh", "y", "c")
GROUPS = ("zl", "zh", "y", "c")
ROUNDS = (
    ((1, 0, 0), (0, 2, 0)),
    ((1, 0, 1), (0, 2, 1)),
    ((1, 1, 0), (0, 3, 0)),
    ((1, 1, 1), (0, 3, 1)),
    ((1, 3, 0), (0, 1, 0)),
    ((1, 3, 1), (0, 1, 1)),
    ((1, 2, 0), (0, 0, 1)),
    ((1, 2, 1), (0, 0, 0)),
)
BATCHES = ((0,), (1, 2), (3, 4), (5, 6, 7))
FINALS = (
    (((0, 0), (0, 1), (1, 0), (1, 1), (2, 0), (2, 1), (3, 0), (3, 1), (7, 1)), False),
    (((4, 0), (4, 1), (5, 0), (5, 1)), True),
    (((6, 0), (6, 1)), True),
    (((7, 0),), True),
)
DEPTH = 3
ANY = pl.BlockSpec(memory_space=pltpu.HBM)
VMEM = pl.BlockSpec(memory_space=pltpu.VMEM)


def ring(step):
    return [(z * 8 + y * 2 + c, (z + step[0]) % 2 * 8 + (y + step[1]) % 4 * 2 + (c + step[2]) % 2) for z, y, c in product(range(2), range(4), range(2))]


def place(step, sign):
    dz, dy, dc = step
    z, y, c = (lax.axis_index(a) for a in SHARD)
    dy = dy if sign > 0 else (4 - dy) % 4
    return lax.rem(z + dz, 2) * 8 + lax.rem(y + dy, 4) * 2 + lax.rem(c + dc, 2)


def in_hbm(x):
    return pltpu.with_memory_space_constraint(x, pltpu.HBM)


def params(mib):
    return pltpu.CompilerParams(vmem_limit_bytes=mib << 20)


def merge_chunks(steps, arrays, earlier=None, router=None):
    _, rows, cols = arrays[0].shape
    n = len(steps)
    last = earlier is not None
    old = [s for _, s in earlier] + list(router) if last else []
    wide = 2 * cols // LANES
    ranks = 16

    def body(*refs):
        ins, refs = refs[:4], refs[4:]
        olds, refs = refs[: len(old)], refs[len(old) :]
        outs, sums, refs = refs[:n], refs[n], refs[n + 1 :]
        bufs, obuf, isem, osem, pay = refs[:4], refs[4], refs[5], refs[6], refs[7]
        copies = []
        for k, s in enumerate(steps):
            e = place(s, 1)
            copies.append([pltpu.make_async_copy(a.at[e], b.at[k], isem.at[k, i]) for i, (a, b) in enumerate(zip(ins, bufs))])
            for c in copies[-1]:
                c.start()
        if last:
            part = (olds[-2][...] * olds[-1][...]).astype(jnp.bfloat16)
            for e in range(sums.shape[0]):
                sums[e, : part.shape[0], :] = part
            for (before, _), o in zip(earlier, olds):
                for k, s in enumerate(before):
                    pay[place(s, 1), :wide, :] = o[k]
        sent = []
        for k, o in enumerate(outs):
            for h in range(2):
                for c in copies[k][2 * h : 2 * h + 2]:
                    c.wait()
                m = bufs[2 * h][k] + bufs[2 * h + 1][k].astype(jnp.float32)
                obuf[k, :, h * cols : (h + 1) * cols] = m.astype(jnp.bfloat16)
                t = jnp.abs(m).reshape(rows // 8, 8, cols).sum(0).sum(0, keepdims=True)
                for j in range(cols // LANES):
                    at = h * (cols // LANES) + j
                    if last:
                        pay[place(steps[k], 1), at : at + 1, :] = t[:, j * LANES : (j + 1) * LANES]
                    else:
                        sums[k, at : at + 1, :] = t[:, j * LANES : (j + 1) * LANES]
            sent.append(pltpu.make_async_copy(obuf.at[k], o, osem.at[k]))
            sent[-1].start()
        if last:
            r = part.shape[0]
            tail = pay[...].astype(jnp.bfloat16)
            for z in range(sums.shape[0] // ranks):
                sums[z * ranks : (z + 1) * ranks, r:, :] = tail
        for c in sent:
            c.wait()

    size = n * rows * cols * 16
    if last:
        r = router[0].shape[0]
        extra = jax.ShapeDtypeStruct((lax.axis_size(GROUPS), 2 * r, LANES), jnp.bfloat16)
        pay = pltpu.VMEM((ranks, r, LANES), jnp.float32)
    else:
        extra = jax.ShapeDtypeStruct((n, wide, LANES), jnp.float32)
        pay = pltpu.VMEM((8, LANES), jnp.float32)
    return pl.pallas_call(
        body,
        in_specs=[ANY] * 4 + [VMEM] * len(old),
        out_specs=[ANY] * n + [VMEM],
        out_shape=[pltpu.HBM((rows, 2 * cols), jnp.bfloat16)] * n + [extra],
        scratch_shapes=[pltpu.VMEM((n, rows, cols), a.dtype) for a in arrays]
        + [pltpu.VMEM((n, rows, 2 * cols), jnp.bfloat16), pltpu.SemaphoreType.DMA((n, 4)), pltpu.SemaphoreType.DMA((n,)), pay],
        compiler_params=params((size >> 20) + 3),
        name="merge",
    )(*[in_hbm(a) for a in arrays], *old)


def finish(steps, chunks, got, before=None, near=False):
    rows, cols = chunks[0].shape
    n, half = len(steps), cols // 2
    wide = cols // LANES
    ranks = 16
    first = before is None
    kept = [] if first else list(before)

    def body(*refs):
        ins, got_ref, refs = refs[:n], refs[n], refs[n + 1 + len(kept) :]
        outs, refs = refs[:2], refs[2:]
        scales, refs = (refs[:2], refs[2:]) if first else (None, refs)
        obuf, osem, *refs = refs
        if not near:
            buf, isem = refs
            copies = [pltpu.make_async_copy(r, buf.at[k], isem.at[k]) for k, r in enumerate(ins)]
            for c in copies:
                c.start()
        mine = got_ref[pl.ds(pl.multiple_of(lax.axis_index("zl") * ranks, ranks), ranks), got_ref.shape[1] // 2 :, :]
        s = mine.astype(jnp.float32).sum(0)[:wide] * (1.0 / D_MODEL)
        if first:
            for j in range(wide):
                a, at = divmod(j * LANES, half)
                scales[a][:, at : at + LANES] = s[j : j + 1, :]
        inv = 1.0 / s
        sent = []
        for k in range(n):
            if not near:
                copies[k].wait()
            to = pl.ds(pl.multiple_of(place(steps[k], -1) * rows, rows), rows)
            for a in range(2):
                for j in range(a * wide // 2, (a + 1) * wide // 2):
                    at = slice(j * LANES, (j + 1) * LANES)
                    x = ins[k][:, at] if near else buf[k, :, at]
                    obuf[k, a, :, j * LANES - a * half : (j + 1) * LANES - a * half] = (x.astype(jnp.float32) * inv[j : j + 1, :]).astype(jnp.bfloat16)
                sent.append(pltpu.make_async_copy(obuf.at[k, a], outs[a].at[to], osem.at[k, a]))
                sent[-1].start()
        for c in sent:
            c.wait()

    full = pltpu.HBM((16 * rows, half), jnp.bfloat16)
    space = pltpu.VMEM if near else pltpu.HBM
    return pl.pallas_call(
        body,
        in_specs=[pl.BlockSpec(memory_space=space)] * n + [VMEM] + [ANY] * len(kept),
        out_specs=[ANY] * 2 + ([VMEM] * 2 if first else []),
        out_shape=[full] * 2 + ([jax.ShapeDtypeStruct((1, half), jnp.float32)] * 2 if first else []),
        scratch_shapes=[pltpu.VMEM((n, 2, rows, half), jnp.bfloat16), pltpu.SemaphoreType.DMA((n, 2))]
        + ([] if near else [pltpu.VMEM((n, rows, cols), jnp.bfloat16), pltpu.SemaphoreType.DMA((n,))]),
        input_output_aliases={} if first else {n + 1: 0, n + 2: 1},
        compiler_params=params(n + 3),
        name="finish",
    )(*[pltpu.with_memory_space_constraint(c, space) for c in chunks], got, *kept)


def lay_router(groups):
    _, s, e, rows = groups[0].shape
    e //= 2
    m = len(groups)

    def body(*refs):
        o_ref, buf = refs[m:]
        x = lax.axis_index("x")
        for k in range(s):
            for d in range(m):
                for w in range(2):
                    at = (w * m + lax.rem(x + m - d, m)) * e
                    buf[k, pl.ds(pl.multiple_of(at, e), e), :] = refs[d][w, k, :e, :].astype(jnp.float32)
            o_ref[k * rows : (k + 1) * rows, :] = buf[k].T.astype(jnp.bfloat16)

    return pl.pallas_call(
        body,
        out_shape=jax.ShapeDtypeStruct((s * rows, 2 * m * e), jnp.bfloat16),
        scratch_shapes=[pltpu.VMEM((s, 2 * m * e, rows), jnp.float32)],
        compiler_params=params(8),
        name="lay_router",
    )(*groups)


def exchange(x, axes):
    return lax.all_to_all(x, axes, 0, 0, tiled=True)


def tied(values, after):
    out = lax.optimization_barrier((*values, *after))
    return list(out[: len(values)]), list(out[len(values) :])


def shards(master_gate, second_gate, master_up, second_up, router_weight, router_gain):
    arrays = [master_gate, second_gate, master_up, second_up]
    chunks, sums = [], []
    for b, batch in enumerate(BATCHES):
        steps = [s for r in batch for s in ROUNDS[r]]
        last = b == len(BATCHES) - 1
        *made, part_sums = merge_chunks(steps, arrays, *((sums, (router_weight.T, router_gain[None])) if last else ()))
        sums.append((steps, part_sums))
        if not last:
            arrays, (made[0],) = tied(arrays, [made[0]])
        for r in batch:
            chunks.append(made[: len(ROUNDS[r])])
            made = made[len(ROUNDS[r]) :]
    small = exchange(sums[-1][1], GROUPS)
    cols = small.reshape(2, 16, *small.shape[1:])
    m = lax.axis_size("x")
    groups = [cols]
    for d in range(1, m):
        groups.append(lax.ppermute(cols, "x", [(i, (i + d) % m) for i in range(m)]))
    router = lay_router(groups)
    got = []
    for r, steps in enumerate(ROUNDS):
        vals = list(chunks[r])
        if r >= DEPTH:
            vals, got[r - DEPTH] = tied(vals, got[r - DEPTH])
        moved = []
        for v, s in zip(vals, steps):
            moved.append(lax.ppermute(v, SHARD, ring(s)) if any(s) else v)
        got.append(moved)
    finals, scales = None, None
    for places, near in FINALS:
        out = finish([ROUNDS[r][i] for r, i in places], [got[r][i] for r, i in places], small, finals, near)
        if finals is None:
            scales = out[2:]
        finals = out[:2]
    return finals[0][None], finals[1][None], *scales, router


def solution(mesh):
    split = Mesh(mesh.devices.reshape(2, 4, 2, 4, 2), ("zl", "x", "zh", "y", "c"))
    w = P(EXPERT, SHARD, None)
    out = P(EXPERT + SHARD, None, None)
    return jax.shard_map(
        shards,
        mesh=split,
        in_specs=(w, w, w, w, P(SHARD, EXPERT), P(SHARD)),
        out_specs=(out, out, P(EXPERT + SHARD, None), P(EXPERT + SHARD, None), P()),
        check_vma=False,
    )
```

```python
from itertools import product

import jax
import jax.numpy as jnp
from jax import lax
from jax.experimental import pallas as pl
from jax.experimental.pallas import tpu as pltpu
from jax.sharding import Mesh
from jax.sharding import PartitionSpec as P


D_MODEL = 2048
LANES = 128
EXPERT = ("zl", "x")
SHARD = ("zh", "y", "c")
GROUPS = ("zl", "zh", "y", "c")
ROUNDS = (
    ((1, 0, 1), (0, 2, 1)),
    ((1, 0, 0), (0, 2, 0)),
    ((1, 1, 1), (0, 3, 1)),
    ((1, 1, 0), (0, 3, 0)),
    ((1, 3, 1), (0, 1, 1)),
    ((1, 3, 0), (0, 1, 0)),
    ((1, 2, 0), (0, 0, 1)),
    ((1, 2, 1), (0, 0, 0)),
)
BATCHES = ((0,), (1, 2), (3, 4), (5, 6, 7))
FINALS = (
    (((0, 0), (0, 1), (1, 0), (1, 1), (2, 0), (2, 1), (3, 0), (3, 1), (7, 1)), False),
    (((4, 0), (4, 1)), True),
    (((5, 0), (5, 1), (6, 0), (6, 1), (7, 0)), True),
)
DEPTH = 3
NEAR = (0, 1, 2)
ANY = pl.BlockSpec(memory_space=pltpu.HBM)
VMEM = pl.BlockSpec(memory_space=pltpu.VMEM)


def ring(step):
    return [(z * 8 + y * 2 + c, (z + step[0]) % 2 * 8 + (y + step[1]) % 4 * 2 + (c + step[2]) % 2) for z, y, c in product(range(2), range(4), range(2))]


def place(step, sign):
    dz, dy, dc = step
    z, y, c = (lax.axis_index(a) for a in SHARD)
    dy = dy if sign > 0 else (4 - dy) % 4
    return lax.rem(z + dz, 2) * 8 + lax.rem(y + dy, 4) * 2 + lax.rem(c + dc, 2)


def in_hbm(x):
    return pltpu.with_memory_space_constraint(x, pltpu.HBM)


def params(mib):
    return pltpu.CompilerParams(vmem_limit_bytes=mib << 20)


def merge_chunks(steps, arrays, earlier=None, router=None, near=False):
    _, rows, cols = arrays[0].shape
    n = len(steps)
    last = earlier is not None
    old = [s for _, s in earlier] + list(router) if last else []
    wide = 2 * cols // LANES
    ranks = 16

    def body(*refs):
        ins, refs = refs[:4], refs[4:]
        olds, refs = refs[: len(old)], refs[len(old) :]
        outs, sums, refs = refs[:n], refs[n], refs[n + 1 :]
        bufs, obuf, isem, osem, pay = refs[:4], refs[4], refs[5], refs[6], refs[7]
        copies = []
        for k, s in enumerate(steps):
            e = place(s, 1)
            copies.append([pltpu.make_async_copy(a.at[e], b.at[k], isem.at[k, i]) for i, (a, b) in enumerate(zip(ins, bufs))])
            for c in copies[-1]:
                c.start()
        if last:
            part = (olds[-2][...] * olds[-1][...]).astype(jnp.bfloat16)
            for e in range(sums.shape[0]):
                sums[e, : part.shape[0], :] = part
            for (before, _), o in zip(earlier, olds):
                for k, s in enumerate(before):
                    pay[place(s, 1), :wide, :] = o[k]
        sent = []
        for k, o in enumerate(outs):
            for h in range(2):
                for c in copies[k][2 * h : 2 * h + 2]:
                    c.wait()
                m = bufs[2 * h][k] + bufs[2 * h + 1][k].astype(jnp.float32)
                to = o if near else obuf.at[k]
                to[:, h * cols : (h + 1) * cols] = m.astype(jnp.bfloat16)
                t = jnp.abs(m).reshape(rows // 8, 8, cols).sum(0).sum(0, keepdims=True)
                for j in range(cols // LANES):
                    at = h * (cols // LANES) + j
                    if last:
                        pay[place(steps[k], 1), at : at + 1, :] = t[:, j * LANES : (j + 1) * LANES]
                    else:
                        sums[k, at : at + 1, :] = t[:, j * LANES : (j + 1) * LANES]
            if not near:
                sent.append(pltpu.make_async_copy(obuf.at[k], o, osem.at[k]))
                sent[-1].start()
        if last:
            r = part.shape[0]
            tail = pay[...].astype(jnp.bfloat16)
            for z in range(sums.shape[0] // ranks):
                sums[z * ranks : (z + 1) * ranks, r:, :] = tail
        for c in sent:
            c.wait()

    size = n * rows * cols * 16
    if last:
        r = router[0].shape[0]
        extra = jax.ShapeDtypeStruct((lax.axis_size(GROUPS), 2 * r, LANES), jnp.bfloat16)
        pay = pltpu.VMEM((ranks, r, LANES), jnp.float32)
    else:
        extra = jax.ShapeDtypeStruct((n, wide, LANES), jnp.float32)
        pay = pltpu.VMEM((8, LANES), jnp.float32)
    return pl.pallas_call(
        body,
        in_specs=[ANY] * 4 + [VMEM] * len(old),
        out_specs=[VMEM if near else ANY] * n + [VMEM],
        out_shape=[(pltpu.VMEM if near else pltpu.HBM)((rows, 2 * cols), jnp.bfloat16)] * n + [extra],
        scratch_shapes=[pltpu.VMEM((n, rows, cols), a.dtype) for a in arrays]
        + [pltpu.VMEM((1 if near else n, rows, 2 * cols), jnp.bfloat16), pltpu.SemaphoreType.DMA((n, 4)), pltpu.SemaphoreType.DMA((n,)), pay],
        compiler_params=params((size >> 20) + 3),
        name="merge",
    )(*[in_hbm(a) for a in arrays], *old)


def finish(steps, chunks, got, before=None, near=False):
    rows, cols = chunks[0].shape
    n, half = len(steps), cols // 2
    wide = cols // LANES
    ranks = 16
    first = before is None
    kept = [] if first else list(before)

    def body(*refs):
        ins, got_ref, refs = refs[:n], refs[n], refs[n + 1 + len(kept) :]
        outs, refs = refs[:2], refs[2:]
        scales, refs = (refs[:2], refs[2:]) if first else (None, refs)
        obuf, osem, *refs = refs
        if not near:
            buf, isem = refs
            copies = [pltpu.make_async_copy(r, buf.at[k], isem.at[k]) for k, r in enumerate(ins)]
            for c in copies:
                c.start()
        mine = got_ref[pl.ds(pl.multiple_of(lax.axis_index("zl") * ranks, ranks), ranks), got_ref.shape[1] // 2 :, :]
        s = mine.astype(jnp.float32).sum(0)[:wide] * (1.0 / D_MODEL)
        if first:
            for j in range(wide):
                a, at = divmod(j * LANES, half)
                scales[a][:, at : at + LANES] = s[j : j + 1, :]
        inv = 1.0 / s
        sent = []
        for k in range(n):
            if not near:
                copies[k].wait()
            to = pl.ds(pl.multiple_of(place(steps[k], -1) * rows, rows), rows)
            for a in range(2):
                for j in range(a * wide // 2, (a + 1) * wide // 2):
                    at = slice(j * LANES, (j + 1) * LANES)
                    x = ins[k][:, at] if near else buf[k, :, at]
                    obuf[k, a, :, j * LANES - a * half : (j + 1) * LANES - a * half] = (x.astype(jnp.float32) * inv[j : j + 1, :]).astype(jnp.bfloat16)
                sent.append(pltpu.make_async_copy(obuf.at[k, a], outs[a].at[to], osem.at[k, a]))
                sent[-1].start()
        for c in sent:
            c.wait()

    full = pltpu.HBM((16 * rows, half), jnp.bfloat16)
    space = pltpu.VMEM if near else pltpu.HBM
    return pl.pallas_call(
        body,
        in_specs=[pl.BlockSpec(memory_space=space)] * n + [VMEM] + [ANY] * len(kept),
        out_specs=[ANY] * 2 + ([VMEM] * 2 if first else []),
        out_shape=[full] * 2 + ([jax.ShapeDtypeStruct((1, half), jnp.float32)] * 2 if first else []),
        scratch_shapes=[pltpu.VMEM((n, 2, rows, half), jnp.bfloat16), pltpu.SemaphoreType.DMA((n, 2))]
        + ([] if near else [pltpu.VMEM((n, rows, cols), jnp.bfloat16), pltpu.SemaphoreType.DMA((n,))]),
        input_output_aliases={} if first else {n + 1: 0, n + 2: 1},
        compiler_params=params(n + 3),
        name="finish",
    )(*[pltpu.with_memory_space_constraint(c, space) for c in chunks], got, *kept)


def lay_router(groups):
    _, s, e, rows = groups[0].shape
    m = len(groups)

    def body(*refs):
        o_ref, buf = refs[m:]
        x = lax.axis_index("x")
        for k in range(s):
            for d in range(m):
                for w in range(2):
                    at = (w * m + lax.rem(x + m - d, m)) * e
                    buf[k, pl.ds(pl.multiple_of(at, e), e), :] = refs[d][w, k].astype(jnp.float32)
            o_ref[k * rows : (k + 1) * rows, :] = buf[k].T.astype(jnp.bfloat16)

    return pl.pallas_call(
        body,
        out_shape=jax.ShapeDtypeStruct((s * rows, 2 * m * e), jnp.bfloat16),
        scratch_shapes=[pltpu.VMEM((s, 2 * m * e, rows), jnp.float32)],
        compiler_params=params(8),
        name="lay_router",
    )(*groups)


def exchange(x, axes):
    return lax.all_to_all(x, axes, 0, 0, tiled=True)


def tied(values, after):
    out = lax.optimization_barrier((*values, *after))
    return list(out[: len(values)]), list(out[len(values) :])


def shards(master_gate, second_gate, master_up, second_up, router_weight, router_gain):
    arrays = [master_gate, second_gate, master_up, second_up]
    chunks, sums = [], []
    for b, batch in enumerate(BATCHES):
        steps = [s for r in batch for s in ROUNDS[r]]
        last = b == len(BATCHES) - 1
        *made, part_sums = merge_chunks(steps, arrays, *((sums, (router_weight.T, router_gain[None])) if last else (None, None)), near=b in NEAR)
        sums.append((steps, part_sums))
        if not last:
            arrays, (made[0],) = tied(arrays, [made[0]])
        for r in batch:
            chunks.append(made[: len(ROUNDS[r])])
            made = made[len(ROUNDS[r]) :]
    small = exchange(sums[-1][1], GROUPS)
    cols = small[:, : small.shape[1] // 2].reshape(2, 16, -1, small.shape[2])
    m = lax.axis_size("x")
    groups = [cols]
    for d in range(1, m):
        groups.append(lax.ppermute(cols, "x", [(i, (i + d) % m) for i in range(m)]))
    router = lay_router(groups)
    got = []
    for r, steps in enumerate(ROUNDS):
        vals = list(chunks[r])
        if r >= DEPTH:
            vals, got[r - DEPTH] = tied(vals, got[r - DEPTH])
        moved = []
        for v, s in zip(vals, steps):
            moved.append(lax.ppermute(v, SHARD, ring(s)) if any(s) else v)
        got.append(moved)
    finals, scales = None, None
    for places, near in FINALS:
        out = finish([ROUNDS[r][i] for r, i in places], [got[r][i] for r, i in places], small, finals, near)
        if finals is None:
            scales = out[2:]
        finals = out[:2]
    return finals[0][None], finals[1][None], *scales, router


def solution(mesh):
    split = Mesh(mesh.devices.reshape(2, 4, 2, 4, 2), ("zl", "x", "zh", "y", "c"))
    w = P(EXPERT, SHARD, None)
    out = P(EXPERT + SHARD, None, None)
    return jax.shard_map(
        shards,
        mesh=split,
        in_specs=(w, w, w, w, P(SHARD, EXPERT), P(SHARD)),
        out_specs=(out, out, P(EXPERT + SHARD, None), P(EXPERT + SHARD, None), P()),
        check_vma=False,
    )
```

```python
from itertools import product

import jax
import jax.numpy as jnp
from jax import lax
from jax.experimental import pallas as pl
from jax.experimental.pallas import tpu as pltpu
from jax.sharding import Mesh
from jax.sharding import PartitionSpec as P


D_MODEL = 2048
LANES = 128
EXPERT = ("zl", "x")
SHARD = ("zh", "y", "c")
GROUPS = ("zl", "zh", "y", "c")
ROUNDS = (
    ((1, 0, 1), (0, 2, 1)),
    ((1, 0, 0), (0, 2, 0)),
    ((1, 1, 0), (0, 3, 0)),
    ((1, 1, 1), (0, 3, 1)),
    ((1, 3, 0), (0, 1, 0)),
    ((1, 3, 1), (0, 1, 1)),
    ((1, 2, 0), (0, 0, 1)),
    ((1, 2, 1), (0, 0, 0)),
)
BATCHES = ((0,), (1, 2), (3, 4), (5, 6, 7))
FINALS = (
    (((0, 0), (0, 1), (1, 0), (1, 1), (2, 0), (2, 1), (3, 0), (3, 1), (7, 1)), False),
    (((4, 0), (4, 1)), True),
    (((5, 0), (5, 1), (6, 0), (6, 1)), True),
    (((7, 0),), True),
)
DEPTH = 3
NEAR = (0, 1, 2, 3)
ANY = pl.BlockSpec(memory_space=pltpu.HBM)
VMEM = pl.BlockSpec(memory_space=pltpu.VMEM)


def ring(step):
    return [(z * 8 + y * 2 + c, (z + step[0]) % 2 * 8 + (y + step[1]) % 4 * 2 + (c + step[2]) % 2) for z, y, c in product(range(2), range(4), range(2))]


def place(step, sign):
    dz, dy, dc = step
    z, y, c = (lax.axis_index(a) for a in SHARD)
    dy = dy if sign > 0 else (4 - dy) % 4
    return lax.rem(z + dz, 2) * 8 + lax.rem(y + dy, 4) * 2 + lax.rem(c + dc, 2)


def in_hbm(x):
    return pltpu.with_memory_space_constraint(x, pltpu.HBM)


def params(mib):
    return pltpu.CompilerParams(vmem_limit_bytes=mib << 20)


def merge_chunks(steps, arrays, earlier=None, router=None, near=False):
    _, rows, cols = arrays[0].shape
    n = len(steps)
    last = earlier is not None
    old = [s for _, s in earlier] + list(router) if last else []
    wide = 2 * cols // LANES
    ranks = 16

    def body(*refs):
        ins, refs = refs[:4], refs[4:]
        olds, refs = refs[: len(old)], refs[len(old) :]
        outs, sums, refs = refs[:n], refs[n], refs[n + 1 :]
        bufs, obuf, isem, osem, pay = refs[:4], refs[4], refs[5], refs[6], refs[7]
        copies = []
        for k, s in enumerate(steps):
            e = place(s, 1)
            copies.append([pltpu.make_async_copy(a.at[e], b.at[k], isem.at[k, i]) for i, (a, b) in enumerate(zip(ins, bufs))])
            for c in copies[-1]:
                c.start()
        if last:
            part = (olds[-2][...] * olds[-1][...]).astype(jnp.bfloat16)
            for e in range(sums.shape[0]):
                sums[e, : part.shape[0], :] = part
            for (before, _), o in zip(earlier, olds):
                for k, s in enumerate(before):
                    pay[place(s, 1), :wide, :] = o[k]
        sent = []
        for k, o in enumerate(outs):
            for h in range(2):
                for c in copies[k][2 * h : 2 * h + 2]:
                    c.wait()
                m = bufs[2 * h][k] + bufs[2 * h + 1][k].astype(jnp.float32)
                to = o if near else obuf.at[k]
                to[:, h * cols : (h + 1) * cols] = m.astype(jnp.bfloat16)
                t = jnp.abs(m).reshape(rows // 8, 8, cols).sum(0).sum(0, keepdims=True)
                for j in range(cols // LANES):
                    at = h * (cols // LANES) + j
                    if last:
                        pay[place(steps[k], 1), at : at + 1, :] = t[:, j * LANES : (j + 1) * LANES]
                    else:
                        sums[k, at : at + 1, :] = t[:, j * LANES : (j + 1) * LANES]
            if not near:
                sent.append(pltpu.make_async_copy(obuf.at[k], o, osem.at[k]))
                sent[-1].start()
        if last:
            r = part.shape[0]
            tail = pay[...].astype(jnp.bfloat16)
            for z in range(sums.shape[0] // ranks):
                sums[z * ranks : (z + 1) * ranks, r:, :] = tail
        for c in sent:
            c.wait()

    size = n * rows * cols * 16
    if last:
        r = router[0].shape[0]
        extra = jax.ShapeDtypeStruct((lax.axis_size(GROUPS), 2 * r, LANES), jnp.bfloat16)
        pay = pltpu.VMEM((ranks, r, LANES), jnp.float32)
    else:
        extra = jax.ShapeDtypeStruct((n, wide, LANES), jnp.float32)
        pay = pltpu.VMEM((8, LANES), jnp.float32)
    return pl.pallas_call(
        body,
        in_specs=[ANY] * 4 + [VMEM] * len(old),
        out_specs=[VMEM if near else ANY] * n + [VMEM],
        out_shape=[(pltpu.VMEM if near else pltpu.HBM)((rows, 2 * cols), jnp.bfloat16)] * n + [extra],
        scratch_shapes=[pltpu.VMEM((n, rows, cols), a.dtype) for a in arrays]
        + [pltpu.VMEM((1 if near else n, rows, 2 * cols), jnp.bfloat16), pltpu.SemaphoreType.DMA((n, 4)), pltpu.SemaphoreType.DMA((n,)), pay],
        compiler_params=params((size >> 20) + 3),
        name="merge",
    )(*[in_hbm(a) for a in arrays], *old)


def finish(steps, chunks, got, before=None, near=False):
    rows, cols = chunks[0].shape
    n, half = len(steps), cols // 2
    wide = cols // LANES
    ranks = 16
    first = before is None
    kept = [] if first else list(before)

    def body(*refs):
        ins, got_ref, refs = refs[:n], refs[n], refs[n + 1 + len(kept) :]
        outs, refs = refs[:2], refs[2:]
        scales, refs = (refs[:2], refs[2:]) if first else (None, refs)
        obuf, osem, *refs = refs
        if not near:
            buf, isem = refs
            copies = [pltpu.make_async_copy(r, buf.at[k], isem.at[k]) for k, r in enumerate(ins)]
            for c in copies:
                c.start()
        mine = got_ref[pl.ds(pl.multiple_of(lax.axis_index("zl") * ranks, ranks), ranks), got_ref.shape[1] // 2 :, :]
        s = mine.astype(jnp.float32).sum(0)[:wide] * (1.0 / D_MODEL)
        if first:
            for j in range(wide):
                a, at = divmod(j * LANES, half)
                scales[a][:, at : at + LANES] = s[j : j + 1, :]
        inv = 1.0 / s
        sent = []
        for k in range(n):
            if not near:
                copies[k].wait()
            to = pl.ds(pl.multiple_of(place(steps[k], -1) * rows, rows), rows)
            for a in range(2):
                for j in range(a * wide // 2, (a + 1) * wide // 2):
                    at = slice(j * LANES, (j + 1) * LANES)
                    x = ins[k][:, at] if near else buf[k, :, at]
                    obuf[k, a, :, j * LANES - a * half : (j + 1) * LANES - a * half] = (x.astype(jnp.float32) * inv[j : j + 1, :]).astype(jnp.bfloat16)
                sent.append(pltpu.make_async_copy(obuf.at[k, a], outs[a].at[to], osem.at[k, a]))
                sent[-1].start()
        for c in sent:
            c.wait()

    full = pltpu.HBM((16 * rows, half), jnp.bfloat16)
    space = pltpu.VMEM if near else pltpu.HBM
    return pl.pallas_call(
        body,
        in_specs=[pl.BlockSpec(memory_space=space)] * n + [VMEM] + [ANY] * len(kept),
        out_specs=[ANY] * 2 + ([VMEM] * 2 if first else []),
        out_shape=[full] * 2 + ([jax.ShapeDtypeStruct((1, half), jnp.float32)] * 2 if first else []),
        scratch_shapes=[pltpu.VMEM((n, 2, rows, half), jnp.bfloat16), pltpu.SemaphoreType.DMA((n, 2))]
        + ([] if near else [pltpu.VMEM((n, rows, cols), jnp.bfloat16), pltpu.SemaphoreType.DMA((n,))]),
        input_output_aliases={} if first else {n + 1: 0, n + 2: 1},
        compiler_params=params(n + 3),
        name="finish",
    )(*[pltpu.with_memory_space_constraint(c, space) for c in chunks], got, *kept)


def lay_router(groups):
    _, s, e, rows = groups[0].shape
    m = len(groups)

    def body(*refs):
        o_ref, buf = refs[m:]
        x = lax.axis_index("x")
        for k in range(s):
            for d in range(m):
                for w in range(2):
                    at = (w * m + lax.rem(x + m - d, m)) * e
                    buf[k, pl.ds(pl.multiple_of(at, e), e), :] = refs[d][w, k].astype(jnp.float32)
            o_ref[k * rows : (k + 1) * rows, :] = buf[k].T.astype(jnp.bfloat16)

    return pl.pallas_call(
        body,
        out_shape=jax.ShapeDtypeStruct((s * rows, 2 * m * e), jnp.bfloat16),
        scratch_shapes=[pltpu.VMEM((s, 2 * m * e, rows), jnp.float32)],
        compiler_params=params(8),
        name="lay_router",
    )(*groups)


def exchange(x, axes):
    return lax.all_to_all(x, axes, 0, 0, tiled=True)


def tied(values, after):
    out = lax.optimization_barrier((*values, *after))
    return list(out[: len(values)]), list(out[len(values) :])


def shards(master_gate, second_gate, master_up, second_up, router_weight, router_gain):
    arrays = [master_gate, second_gate, master_up, second_up]
    chunks, sums = [], []
    for b, batch in enumerate(BATCHES):
        steps = [s for r in batch for s in ROUNDS[r]]
        last = b == len(BATCHES) - 1
        *made, part_sums = merge_chunks(steps, arrays, *((sums, (router_weight.T, router_gain[None])) if last else (None, None)), near=b in NEAR)
        sums.append((steps, part_sums))
        if not last:
            arrays, (made[0],) = tied(arrays, [made[0]])
        for r in batch:
            chunks.append(made[: len(ROUNDS[r])])
            made = made[len(ROUNDS[r]) :]
    small = exchange(sums[-1][1], GROUPS)
    cols = small[:, : small.shape[1] // 2].reshape(2, 16, -1, small.shape[2])
    m = lax.axis_size("x")
    groups = [cols]
    for d in range(1, m):
        groups.append(lax.ppermute(cols, "x", [(i, (i + d) % m) for i in range(m)]))
    router = lay_router(groups)
    got = []
    for r, steps in enumerate(ROUNDS):
        vals = list(chunks[r])
        if r >= DEPTH:
            vals, got[r - DEPTH] = tied(vals, got[r - DEPTH])
        moved = []
        for v, s in zip(vals, steps):
            moved.append(lax.ppermute(v, SHARD, ring(s)) if any(s) else v)
        got.append(moved)
    finals, scales = None, None
    for places, near in FINALS:
        out = finish([ROUNDS[r][i] for r, i in places], [got[r][i] for r, i in places], small, finals, near)
        if finals is None:
            scales = out[2:]
        finals = out[:2]
    return finals[0][None], finals[1][None], *scales, router


def solution(mesh):
    split = Mesh(mesh.devices.reshape(2, 4, 2, 4, 2), ("zl", "x", "zh", "y", "c"))
    w = P(EXPERT, SHARD, None)
    out = P(EXPERT + SHARD, None, None)
    return jax.shard_map(
        shards,
        mesh=split,
        in_specs=(w, w, w, w, P(SHARD, EXPERT), P(SHARD)),
        out_specs=(out, out, P(EXPERT + SHARD, None), P(EXPERT + SHARD, None), P()),
        check_vma=False,
    )
```
